32 devices in a mesh: section: 4 (over y, x), dp: 8 (over z, core).
Axes of the slice: x: 2, y: 2, z: 4, core: 2. Of those that a mesh axis runs over, the one named last changes fastest.
Arguments:
- patches: bfloat16 [2048, 1536], P('dp'), may hold values from -6 to 6
- w_gate: bfloat16 [4, 1536, 2048], P('section'), may hold values from -0.15625 to 0.15625
- w_up: bfloat16 [4, 1536, 2048], P('section'), may hold values from -0.15625 to 0.15625
- w_down: bfloat16 [4, 2048, 1536], P('section'), may hold values from -0.125 to 0.125
- w_proj: bfloat16 [1536, 768], P(None, 'section'), may hold values from -0.15625 to 0.15625
- slide_of: int32 [8, 1], replicated, may hold values from 0 to 7
- tile_pos: int32 [8], replicated, may hold values from 0 to 1023
- slide_cot: float32 [8, 768], P('dp', 'section'), may hold values from -6 to 6
Outputs:
- slide_embed: float32 [8, 768], P('dp', 'section')
- grad_gate: float32 [4, 1536, 2048], P('section', 'dp')
- grad_up: float32 [4, 1536, 2048], P('section', 'dp')
- grad_down: float32 [4, 2048, 1536], P('section', 'dp')
- grad_proj: float32 [1536, 768], P('dp', 'section')
The draws below stay inside these ranges and needn't reach their ends.
Inputs may be any that keep to these rules, and one draw needn't show every extreme that they name: `slide_of`: every slide has at least one tile.
All inputs are finite; a program needn't handle non-finite values.
Results may differ from the reference program's by a relative error of at most 0.025.
Values may be sent and summed in bfloat16 or wider, within the bound.
No kernel may reach another device: no remote copies, remote signals or barrier semaphores. Data moves between devices by JAX's collectives and lax.ppermute only.
A program may use at most 128 MiB of HBM per device.

```python
import math
import jax
import jax.numpy as jnp
from jax import lax

D = 1536
SW = 768
FFW = 2048
PATCH = 256
GRID = 1024
TILE_DEV = 1
SECTIONS = 4
TILES = 8
SLIDES = 8
TOKENS = 2048
N_DP = 8


def plant(array, key, smallest, largest):
    spot = [jax.random.randint(jax.random.fold_in(key, axis), (), 0, length) for axis, length in enumerate(array.shape)]
    main_axis = array.shape.index(max(array.shape))
    next_to = spot[:main_axis] + [(spot[main_axis] + 1) % array.shape[main_axis]] + spot[main_axis + 1:]
    return array.at[tuple(spot)].set(smallest).at[tuple(next_to)].set(largest)


def block_levels(key, dims, split, low, top_value):
    level = 1.0
    for dim, parts in split:
        heights = jax.random.uniform(jax.random.fold_in(jax.random.fold_in(key, 6), dim), (parts,), jnp.float32, low / len(split), top_value / len(split))
        level = level * jnp.repeat(jnp.exp(heights), dims[dim] // parts).reshape((-1,) + (1,) * (len(dims) - 1 - dim))
    return level


def choose_distinct(stream_key, rows, number_of, top, lift):
    order = jax.random.permutation(jax.random.fold_in(stream_key, 1), number_of)
    favour = order
    for power in range(3):
        favour = favour * favour // number_of
    favour = favour * lift // number_of
    tickets = jax.random.randint(jax.random.fold_in(stream_key, 2), (rows, number_of), 0, 4096) + favour
    holders = jax.random.permutation(jax.random.fold_in(stream_key, 3), rows)[jnp.arange(number_of) % rows]
    tickets = jnp.where(jnp.arange(rows)[:, None] == holders[None, :], 1 << 14, tickets)
    priority = tickets * number_of + jnp.arange(number_of)
    return lax.top_k(priority.astype(jnp.int32), top)[1].astype(jnp.int32)


def bell_draw(stream_key, shape, deviation, bound, cuts=(), held_as=jnp.bfloat16):
    result = deviation * jax.random.normal(stream_key, shape, jnp.float32)
    if cuts:
        result = result * block_levels(stream_key, shape, cuts, -0.22, 0.18)
    return jnp.clip(result, -bound, bound).astype(held_as)


def setup_inputs(seed: int = 0) -> dict:
    arg_keys = jax.random.split(jax.random.key(seed), 9)
    patches = bell_draw(arg_keys[0], (TOKENS, D), 1.0, 6.0, ((0, 8),))
    w_gate = bell_draw(arg_keys[1], (SECTIONS, D, FFW), D ** -0.5, 0.15625, ((0, 4),))
    w_up = bell_draw(arg_keys[2], (SECTIONS, D, FFW), D ** -0.5, 0.15625, ((0, 4),))
    w_down = bell_draw(arg_keys[3], (SECTIONS, FFW, D), FFW ** -0.5, 0.125, ((0, 4),))
    w_proj = bell_draw(arg_keys[4], (D, SW), D ** -0.5, 0.15625, ((1, 4),))
    slide_of = choose_distinct(arg_keys[5], TILES, SLIDES, 1, 2048)
    tile_pos = plant(jax.random.randint(arg_keys[6], (TILES,), 0, GRID), jax.random.fold_in(arg_keys[6], 1), 0, GRID - 1).astype(jnp.int32)
    slide_cot = bell_draw(arg_keys[7], (SLIDES, SW), 1.0, 6.0, ((0, 8), (1, 4)), jnp.float32)
    return {"patches": patches, "w_gate": w_gate, "w_up": w_up, "w_down": w_down, "w_proj": w_proj, "slide_of": slide_of, "tile_pos": tile_pos, "slide_cot": slide_cot}


EPS = 1e-06

def normalize(values):
    center = values - lax.optimization_barrier(jnp.mean(values, axis=-1, keepdims=True))
    inverse = lax.rsqrt(lax.optimization_barrier(jnp.mean(center * center, axis=-1, keepdims=True)) + EPS)
    return (center * inverse, inverse)

def norm_back(grad, normed, inverse):
    return inverse * (grad - lax.optimization_barrier(jnp.mean(grad, axis=-1, keepdims=True)) - normed * lax.optimization_barrier(jnp.mean(grad * normed, axis=-1, keepdims=True)))

def position_table(positions, first, count, total):
    column = first + jnp.arange(count, dtype=jnp.int32)
    freq = jnp.exp(-(2 * (column // 2)).astype(jnp.float32) * (math.log(10000.0) / total))
    angle = positions.astype(jnp.float32)[:, None] * freq[None, :]
    return jnp.where((column % 2 == 0)[None, :], jnp.sin(angle), jnp.cos(angle))

def contract_rows(left, right):
    return lax.dot_general(left, right, (((0,), (0,)), ((), ())), preferred_element_type=jnp.float32)

def contract_cols(left, right):
    return lax.dot_general(left, right, (((1,), (1,)), ((), ())), preferred_element_type=jnp.float32)

def derivative(values):
    sig = jax.nn.sigmoid(values)
    return sig * (1.0 + values * (1.0 - sig))

def reference(patches, w_gate, w_up, w_down, w_proj, slide_of, tile_pos, slide_cot):
    state = patches
    inputs = []
    for section in range(SECTIONS):
        normed, inverse = normalize(state.astype(jnp.float32))
        hidden = normed.astype(jnp.bfloat16)
        gate = jnp.dot(hidden, w_gate[section], preferred_element_type=jnp.float32)
        upper = jnp.dot(hidden, w_up[section], preferred_element_type=jnp.float32)
        active = (jax.nn.silu(gate) * upper).astype(jnp.bfloat16)
        output = jnp.dot(active, w_down[section], preferred_element_type=jnp.float32)
        inputs.append(state)
        state = (state.astype(jnp.float32) + output).astype(jnp.bfloat16)
    pooled = lax.optimization_barrier(jnp.mean(state.astype(jnp.float32).reshape(TILES, PATCH, D), axis=1))
    tile_norm, inv_tile = normalize(pooled)
    embed = tile_norm.astype(jnp.bfloat16)
    pre = jnp.dot(embed, w_proj, preferred_element_type=jnp.float32) + position_table(tile_pos, 0, SW, SW)
    member = (slide_of[:, 0][None, :] == jnp.arange(SLIDES, dtype=jnp.int32)[:, None]).astype(jnp.float32)
    counts = lax.optimization_barrier(jnp.sum(member, axis=1))
    slide_embed = jnp.dot(member, jax.nn.silu(pre), precision=lax.Precision.HIGHEST) / counts[:, None]
    back = jnp.dot(member.T, slide_cot / counts[:, None], precision=lax.Precision.HIGHEST)
    dpre = (back * derivative(pre)).astype(jnp.bfloat16)
    grad_proj = contract_rows(embed, dpre)
    dembed = contract_cols(dpre, w_proj)
    dpooled = norm_back(dembed, tile_norm, inv_tile)
    grad_state = jnp.repeat(dpooled / PATCH, PATCH, axis=0).astype(jnp.bfloat16)
    rows = TILE_DEV * PATCH
    grads_gate = [None] * SECTIONS
    grads_up = [None] * SECTIONS
    grads_down = [None] * SECTIONS
    for section in reversed(range(SECTIONS)):
        state = inputs[section]
        normed, inverse = normalize(state.astype(jnp.float32))
        hidden = normed.astype(jnp.bfloat16)
        gate = jnp.dot(hidden, w_gate[section], preferred_element_type=jnp.float32)
        upper = jnp.dot(hidden, w_up[section], preferred_element_type=jnp.float32)
        active = (jax.nn.silu(gate) * upper).astype(jnp.bfloat16)
        dact = contract_cols(grad_state, w_down[section])
        dgate = (dact * upper * derivative(gate)).astype(jnp.bfloat16)
        dupper = (dact * jax.nn.silu(gate)).astype(jnp.bfloat16)
        dhid = contract_cols(dgate, w_gate[section]) + contract_cols(dupper, w_up[section])
        new_grad = (grad_state.astype(jnp.float32) + norm_back(dhid, normed, inverse)).astype(jnp.bfloat16)

        def group_sum(carry, pieces):
            p_hidden, p_dgate, p_dupper, p_active, p_grad = pieces
            terms = (contract_rows(p_hidden, p_dgate), contract_rows(p_hidden, p_dupper), contract_rows(p_active, p_grad))
            rounded = tuple((lax.optimization_barrier(term.astype(jnp.bfloat16)).astype(jnp.float32) for term in terms))
            return (tuple((c + r for c, r in zip(carry, rounded))), None)
        zeros_in = jnp.zeros((D, FFW), jnp.float32)
        zeros_out = jnp.zeros((FFW, D), jnp.float32)
        pieces = (hidden.reshape(N_DP, rows, D), dgate.reshape(N_DP, rows, FFW), dupper.reshape(N_DP, rows, FFW), active.reshape(N_DP, rows, FFW), grad_state.reshape(N_DP, rows, D))
        sums, _ = lax.scan(group_sum, (zeros_in, zeros_in, zeros_out), pieces)
        grads_gate[section], grads_up[section], grads_down[section] = sums
        grad_state = new_grad
    return (slide_embed, jnp.stack(grads_gate), jnp.stack(grads_up), jnp.stack(grads_down), grad_proj)
```

```python
import functools
import math

import jax
import jax.numpy as jnp
from jax import lax
from jax.experimental import pallas as pl
from jax.experimental.pallas import tpu as pltpu
from jax.sharding import PartitionSpec as P

PATCH = 256


EPS = 1e-06
BF = jnp.bfloat16
F32 = jnp.float32
ANY = pl.BlockSpec(memory_space=pl.ANY)


def normalize(values):
    center = values - jnp.mean(values, axis=-1, keepdims=True)
    inverse = lax.rsqrt(jnp.mean(center * center, axis=-1, keepdims=True) + EPS)
    return (center * inverse, inverse)


def norm_back(grad, normed, inverse):
    return inverse * (
        grad
        - jnp.mean(grad, axis=-1, keepdims=True)
        - normed * jnp.mean(grad * normed, axis=-1, keepdims=True)
    )


def position_table(positions, first, count, total):
    column = first + jnp.arange(count, dtype=jnp.int32)
    freq = jnp.exp(-(2 * (column // 2)).astype(jnp.float32) * (math.log(10000.0) / total))
    angle = positions.astype(jnp.float32)[:, None] * freq[None, :]
    return jnp.where((column % 2 == 0)[None, :], jnp.sin(angle), jnp.cos(angle))


def dot_rows(left, right):
    return lax.dot_general(left, right, (((0,), (0,)), ((), ())), preferred_element_type=F32)


def dot_cols(left, right):
    return lax.dot_general(left, right, (((1,), (1,)), ((), ())), preferred_element_type=F32)


def dot(left, right):
    return jnp.dot(left, right, preferred_element_type=F32)


def derivative(values):
    sig = jax.nn.sigmoid(values)
    return sig * (1.0 + values * (1.0 - sig))


def after(value, *earlier):
    return lax.optimization_barrier((value, *earlier))[0]


def gate_terms(hidden, w_gate, w_up):
    gate = dot(hidden, w_gate)
    upper = dot(hidden, w_up)
    sig = jax.nn.sigmoid(gate)
    silu = gate * sig
    return ((silu * upper).astype(BF), silu.astype(BF), (upper * (sig * (1.0 + gate * (1.0 - sig)))).astype(BF))


TOKEN = jax.ShapeDtypeStruct((8, 128), F32)
TOKEN_SPEC = pl.BlockSpec((8, 128), lambda i, p: (0, 0))


def cost(flops, bytes_accessed):
    return pl.CostEstimate(flops=int(flops), bytes_accessed=int(bytes_accessed), transcendentals=0)


def forward_kernel(flags, dep, inc, fresh, wg, wu, wd, *refs):
    out, sx, a_out, b_out, sums, tok, hid, acc = refs[-8:]
    i = pl.program_id(0)
    running = flags[0] == 1

    @pl.when(i == 0)
    def _():
        tok[...] = jnp.zeros_like(tok)

    @pl.when(running & (i == 0))
    def _():
        @pl.when(flags[2] == 1)
        def _():
            sx[0] = fresh[0]

        @pl.when(flags[2] == 0)
        def _():
            sx[0] = inc[...]

        state = sx[0].astype(F32)
        hid[...] = normalize(state)[0].astype(BF)
        acc[...] = state

    @pl.when(running)
    def _():
        active, a, b = gate_terms(hid[...], wg[...], wu[...])
        a_out[0] = a
        b_out[0] = b
        acc[...] += dot(active, wd[...])

    @pl.when(running & (i == pl.num_programs(0) - 1))
    def _():
        result = acc[...].astype(BF)
        out[...] = result
        sums[0] = jnp.sum(result.astype(F32), axis=0, keepdims=True)


def forward_step(flags, dep, inc, fresh, weights, saved, chunk=256):
    n, rows, width = fresh.shape
    ffw = weights[0].shape[1]
    slots = n + 1
    pick = lambda i, p: jnp.where(p[0] == 1, i, 0)
    slot_chunk = pl.BlockSpec((1, rows, chunk), lambda i, p: (p[1], 0, pick(i, p)))
    slot_state = pl.BlockSpec((1, rows, width), lambda i, p: (p[1], 0, 0))
    whole = pl.BlockSpec((rows, width), lambda i, p: (0, 0))
    out, *saved, tok = pl.pallas_call(
        forward_kernel,
        grid_spec=pltpu.PrefetchScalarGridSpec(
            num_scalar_prefetch=1,
            grid=(ffw // chunk,),
            in_specs=[
                ANY,
                whole,
                pl.BlockSpec((1, rows, width), lambda i, p: (jnp.minimum(p[1], n - 1), 0, 0)),
                pl.BlockSpec((width, chunk), lambda i, p: (0, pick(i, p))),
                pl.BlockSpec((width, chunk), lambda i, p: (0, pick(i, p))),
                pl.BlockSpec((chunk, width), lambda i, p: (pick(i, p), 0)),
            ]
            + [ANY] * len(saved),
            out_specs=[
                whole,
                slot_state,
                slot_chunk,
                slot_chunk,
                pl.BlockSpec((1, 1, width), lambda i, p: (p[1], 0, 0)),
                TOKEN_SPEC,
            ],
            scratch_shapes=[pltpu.VMEM((rows, width), BF), pltpu.VMEM((rows, width), F32)],
        ),
        out_shape=[
            jax.ShapeDtypeStruct((rows, width), BF),
            jax.ShapeDtypeStruct((slots, rows, width), BF),
            jax.ShapeDtypeStruct((slots, rows, ffw), BF),
            jax.ShapeDtypeStruct((slots, rows, ffw), BF),
            jax.ShapeDtypeStruct((slots, 1, width), F32),
            TOKEN,
        ],
        input_output_aliases={7 + k: 1 + k for k in range(len(saved))},
        cost_estimate=cost(6 * rows * width * ffw, 6 * width * ffw),
        name="forward_step",
    )(flags, dep, inc, fresh, *weights, *saved)
    return out, tuple(saved), tok


def backward_kernel(flags, dep, inc, start, sx, a_in, b_in, wg, wu, wd, *refs):
    out, g_out, d_out, tok, grad, acc = refs[-6:]
    i = pl.program_id(0)
    running = flags[0] == 1
    passing = flags[3] == 1

    @pl.when(i == 0)
    def _():
        tok[...] = jnp.zeros_like(tok)

    @pl.when(running & (i == 0))
    def _():
        @pl.when(flags[2] == 1)
        def _():
            grad[...] = jnp.broadcast_to(start[0], grad.shape)

        @pl.when(flags[2] == 0)
        def _():
            grad[...] = inc[...]

        g_out[0] = grad[...]
        acc[...] = jnp.zeros_like(acc)

    @pl.when(passing)
    def _():
        dact = dot_cols(grad[...], wd[...])
        dgate = (dact * b_in[0]).astype(BF)
        dupper = (dact * a_in[0]).astype(BF)
        acc[...] += dot_cols(dgate, wg[...]) + dot_cols(dupper, wu[...])

    @pl.when(passing & (i == pl.num_programs(0) - 1))
    def _():
        normed, inverse = normalize(sx[0].astype(F32))
        result = (grad[...].astype(F32) + norm_back(acc[...], normed, inverse)).astype(BF)
        out[...] = result
        d_out[0] = result


def backward_step(flags, dep, inc, start, saved, weights, kept, chunk=256):
    sx, a, b, _ = saved
    rows, width = inc.shape
    n = sx.shape[0] - 1
    per_tile = n // start.shape[0]
    ffw = weights[0].shape[1]
    pick = lambda i, p: jnp.where(p[3] == 1, i, 0)
    slot_chunk = pl.BlockSpec((1, rows, chunk), lambda i, p: (p[1], 0, pick(i, p)))
    slot_state = pl.BlockSpec((1, rows, width), lambda i, p: (p[1], 0, 0))
    whole = pl.BlockSpec((rows, width), lambda i, p: (0, 0))
    out, *kept, tok = pl.pallas_call(
        backward_kernel,
        grid_spec=pltpu.PrefetchScalarGridSpec(
            num_scalar_prefetch=1,
            grid=(ffw // chunk,),
            in_specs=[
                ANY,
                whole,
                pl.BlockSpec((1, 1, width), lambda i, p: (jnp.minimum(p[1], n - 1) // per_tile, 0, 0)),
                slot_state,
                slot_chunk,
                slot_chunk,
                pl.BlockSpec((width, chunk), lambda i, p: (0, pick(i, p))),
                pl.BlockSpec((width, chunk), lambda i, p: (0, pick(i, p))),
                pl.BlockSpec((chunk, width), lambda i, p: (pick(i, p), 0)),
            ]
            + [ANY] * len(kept),
            out_specs=[whole, slot_state, slot_state, TOKEN_SPEC],
            scratch_shapes=[pltpu.VMEM((rows, width), BF), pltpu.VMEM((rows, width), F32)],
        ),
        out_shape=[
            jax.ShapeDtypeStruct((rows, width), BF),
            jax.ShapeDtypeStruct(sx.shape, BF),
            jax.ShapeDtypeStruct(sx.shape, BF),
            TOKEN,
        ],
        input_output_aliases={10 + k: 1 + k for k in range(len(kept))},
        cost_estimate=cost(6 * rows * width * ffw, 6 * width * ffw),
        name="backward_step",
    )(flags, dep, inc, start, sx, a, b, *weights, *kept)
    return out, tuple(kept), tok


def terms_kernel(pieces, shared, first, flags, dep, *refs):
    sources = refs[:pieces]
    wg, wu = refs[pieces : pieces + 2]
    rest = refs[pieces + 2 :]
    if not first:
        rest = rest[4:]
    a_out, b_out, act, hid_out, tok, state, hid, sems = rest
    i = pl.program_id(0)
    running = flags[0] == 1
    share = hid_out.shape[2]
    step = sources[0].shape[0]

    @pl.when(i == 0)
    def _():
        tok[...] = jnp.zeros_like(tok)

    @pl.when(running & (i == 0))
    def _():
        copies = [
            pltpu.make_async_copy(source, state.at[pl.ds(k * step, step)], sems.at[k])
            for k, source in enumerate(sources)
        ]
        for copy in copies:
            copy.start()
        for k, copy in enumerate(copies):
            copy.wait()
            span = pl.ds(k * step, step)
            hid[span] = normalize(state[span].astype(F32))[0].astype(BF)
        if shared:
            hid_out[0] = hid[:, pl.ds(pl.multiple_of(flags[1] * share, 128), share)]
        else:
            hid_out[0] = hid[...]

    @pl.when(running)
    def _():
        for k in range(pieces):
            span = pl.ds(k * step, step)
            active, a, b = gate_terms(hid[span], wg[...], wu[...])
            a_out[0, span] = a
            b_out[0, span] = b
            if shared:

                @pl.when(i == flags[1])
                def _():
                    act[0, span] = active
            else:
                act[0, span] = active


def all_terms(flags, dep, sources, weights, share, chunk, previous=None):
    pieces = len(sources)
    step, width = sources[0].shape
    tokens = pieces * step
    ffw = weights[0].shape[1]
    parts = ffw // chunk
    shared = share < width
    pick = lambda i, p: jnp.where(p[0] == 1, i, 0)
    junk = lambda i, p: jnp.where(p[0] == 1, i, parts)
    one = lambda i, p: jnp.where(p[0] == 1, 0, 1)
    act_map = (lambda i, p: (one(i, p), 0, 0)) if shared else (lambda i, p: (one(i, p), 0, pick(i, p)))
    shapes = [
        jax.ShapeDtypeStruct((parts + 1, tokens, chunk), BF),
        jax.ShapeDtypeStruct((parts + 1, tokens, chunk), BF),
        jax.ShapeDtypeStruct((2, tokens, chunk if shared else ffw), BF),
        jax.ShapeDtypeStruct((2, tokens, share), BF),
        TOKEN,
    ]
    extra = [] if previous is None else list(previous)
    base = 2 + pieces + 2
    *outs, tok = pl.pallas_call(
        functools.partial(terms_kernel, pieces, shared, previous is None),
        grid_spec=pltpu.PrefetchScalarGridSpec(
            num_scalar_prefetch=1,
            grid=(parts,),
            in_specs=[ANY]
            + [ANY] * pieces
            + [pl.BlockSpec((width, chunk), lambda i, p: (0, pick(i, p)))] * 2
            + [ANY] * len(extra),
            out_specs=[
                pl.BlockSpec((1, tokens, chunk), lambda i, p: (junk(i, p), 0, 0)),
                pl.BlockSpec((1, tokens, chunk), lambda i, p: (junk(i, p), 0, 0)),
                pl.BlockSpec((1, tokens, chunk), act_map),
                pl.BlockSpec((1, tokens, share), lambda i, p: (one(i, p), 0, 0)),
                TOKEN_SPEC,
            ],
            scratch_shapes=[
                pltpu.VMEM((tokens, width), BF),
                pltpu.VMEM((tokens, width), BF),
                pltpu.SemaphoreType.DMA((pieces,)),
            ],
        ),
        out_shape=shapes,
        input_output_aliases={base + k: k for k in range(len(extra))},
        cost_estimate=cost(4 * tokens * width * ffw, 4 * width * ffw + 4 * tokens * ffw),
        name="all_terms",
    )(flags, dep, *sources, weights[0], weights[1], *extra)
    return tuple(outs), tok


def gradients_kernel(pieces, *refs):
    sources = refs[:pieces]
    a_in, b_in, act, hid, wd, gg, gu, gd, grad, dgate, dupper, sems = refs[pieces:]
    i = pl.program_id(0)
    step = sources[0].shape[0]
    tokens = grad.shape[0]
    span_rows = min(256, tokens)

    @pl.when(i == 0)
    def _():
        copies = [
            pltpu.make_async_copy(source, grad.at[pl.ds(k * step, step)], sems.at[k])
            for k, source in enumerate(sources)
        ]
        for copy in copies:
            copy.start()
        for copy in copies:
            copy.wait()

    for k in range(tokens // span_rows):
        span = pl.ds(k * span_rows, span_rows)
        dact = dot_cols(grad[span], wd[...])
        dgate[span] = (dact * b_in[0, span]).astype(BF)
        dupper[span] = (dact * a_in[0, span]).astype(BF)
    gg[...] = dot_rows(hid[0], dgate[...]).astype(BF)
    gu[...] = dot_rows(hid[0], dupper[...]).astype(BF)
    part = gd.shape[1]
    gd[...] = dot_rows(act[0], grad[:, pl.ds(pl.multiple_of(i * part, 128), part)]).astype(BF)


def gradients(sources, terms, w_down):
    a, b, act, hid = terms
    pieces = len(sources)
    step, width = sources[0].shape
    tokens = pieces * step
    chunk = a.shape[2]
    ffw = w_down.shape[0]
    parts = ffw // chunk
    return pl.pallas_call(
        functools.partial(gradients_kernel, pieces),
        grid=(parts,),
        in_specs=[ANY] * pieces
        + [
            pl.BlockSpec((1, tokens, chunk), lambda i: (i, 0, 0)),
            pl.BlockSpec((1, tokens, chunk), lambda i: (i, 0, 0)),
            pl.BlockSpec((1, tokens, act.shape[2]), lambda i: (0, 0, 0)),
            pl.BlockSpec((1, tokens, hid.shape[2]), lambda i: (0, 0, 0)),
            pl.BlockSpec((chunk, width), lambda i: (i, 0)),
        ],
        out_specs=[
            pl.BlockSpec((hid.shape[2], chunk), lambda i: (0, i)),
            pl.BlockSpec((hid.shape[2], chunk), lambda i: (0, i)),
            pl.BlockSpec((act.shape[2], width // parts), lambda i: (0, i)),
        ],
        out_shape=[
            jax.ShapeDtypeStruct((hid.shape[2], ffw), BF),
            jax.ShapeDtypeStruct((hid.shape[2], ffw), BF),
            jax.ShapeDtypeStruct((act.shape[2], width), BF),
        ],
        scratch_shapes=[
            pltpu.VMEM((tokens, width), BF),
            pltpu.VMEM((tokens, chunk), BF),
            pltpu.VMEM((tokens, chunk), BF),
            pltpu.SemaphoreType.DMA((pieces,)),
        ],
        cost_estimate=cost(
            2 * tokens * (width * ffw + 2 * hid.shape[2] * ffw + act.shape[2] * width), 2 * width * ffw + 4 * tokens * ffw
        ),
        name="gradients",
    )(*sources, a, b, act, hid, w_down)


def double_up(rows, axis):
    size = lax.axis_size(axis)
    have = 1
    while have < size:
        take = min(have, size - have)
        piece = rows[: take * (rows.shape[0] // have)]
        moved = lax.ppermute(piece, axis, [(i, (i - have) % size) for i in range(size)])
        rows = jnp.concatenate([rows, moved], axis=0)
        have += take
    return rows


def local(patches, w_gate, w_up, w_down, w_proj, slide_of, tile_pos, slide_cot):
    sections = lax.axis_size("section")
    groups = lax.axis_size("dp")
    section = lax.axis_index("section")
    group = lax.axis_index("dp")
    last = sections - 1
    is_last = section == last
    weights = (w_gate[0], w_up[0], w_down[0])
    rows_all, width = patches.shape
    ffw = w_gate.shape[2]
    block = PATCH // 2
    blocks = rows_all // block
    tiles = rows_all // PATCH
    steps = blocks + sections - 1
    features = w_proj.shape[1]
    pairs = groups // 2
    relay = groups % 2 == 0 and (2 * width // groups) % 128 == 0 and (2 * ffw // groups) % 128 == 0
    relay = relay and pairs >= 2 and pairs * rows_all <= 1024
    both = ("section", "dp")

    def shift(value, distance, which):
        route = [
            (s * groups + 2 * z + c, s * groups + 2 * ((z + distance) % pairs) + c)
            for s in which
            for z in range(pairs)
            for c in range(2)
        ]
        return lax.ppermute(value, both, route)

    def to_last(value):
        return [lax.ppermute(value, "section", [(s, last)]) for s in range(last)]

    fresh = patches.reshape(blocks, block, width)
    saved = ()
    incoming = fresh[0]
    tok = slide_cot
    early = None
    for step in range(steps):
        position = step - section
        running = (position >= 0) & (position < blocks)
        flags = jnp.stack([running, jnp.where(running, position, blocks), section == 0]).astype(jnp.int32)
        output, saved, tok = forward_step(flags, tok, incoming, fresh, weights, saved)
        route = [(s, s + 1) for s in range(last) if 0 <= step - s < blocks]
        if route:
            incoming = lax.ppermute(output, "section", route)
        if step == blocks - 1:
            early = tok
    others = tuple(range(1, sections))
    if relay:
        source = after(patches, early)
        first_rows = [source] + [shift(source, d, (0,)) for d in range(1, pairs)]
        own = saved[0][:blocks].reshape(rows_all, width)
        later_rows = [own] + [shift(own, d, others) for d in range(1, pairs)]
    else:
        later_rows = [saved[0][:blocks].reshape(rows_all, width)]
    w_early, cot_early = lax.optimization_barrier((w_proj, slide_cot, early))[:2]
    cot_rows = double_up(cot_early, "dp")
    w_full = jnp.concatenate(to_last(w_early) + [w_proj], axis=1)
    cot_full = jnp.concatenate(to_last(cot_rows) + [cot_rows], axis=1)

    slides = slide_cot.shape[0]
    ring = (group + jnp.arange(groups, dtype=jnp.int32)) % groups
    slide_ids = (ring[:, None] * slides + jnp.arange(slides, dtype=jnp.int32)[None]).reshape(-1)
    tile_ids = (ring[:, None] * tiles + jnp.arange(tiles, dtype=jnp.int32)[None]).reshape(-1)
    tile_slide = slide_of[:, 0]
    counts = jnp.sum((tile_slide[None] == slide_ids[:, None]).astype(F32), axis=1)

    def back_rows(tile_index, cots):
        member = (jnp.take(tile_slide, tile_index)[:, None] == slide_ids[None]).astype(F32)
        return jnp.dot(member, cots / counts[:, None], precision=lax.Precision.HIGHEST)

    own_tiles = group * tiles + jnp.arange(tiles, dtype=jnp.int32)
    own_pos = lax.dynamic_slice_in_dim(tile_pos, group * tiles, tiles)
    total = features * sections
    own_back = back_rows(own_tiles, cot_full)
    own_table = position_table(own_pos, 0, total, total)
    pooled = jnp.sum(saved[3][:blocks].reshape(tiles, blocks // tiles, width), axis=1) / PATCH
    tile_norm, inv_tile = normalize(pooled)
    embed = tile_norm.astype(BF)
    pre = dot(embed, w_full) + own_table
    dpre = (own_back * derivative(pre)).astype(BF)
    dembed = dot_cols(dpre, w_full)
    dpooled = norm_back(dembed, tile_norm, inv_tile)
    start = (dpooled / PATCH).astype(BF).reshape(tiles, 1, width)

    kept = ()
    incoming = fresh[0]
    share = 2 * width // groups if relay else width
    chunk = 2 * ffw // groups if relay else min(512, ffw)
    terms = None
    received = [[None] * pairs for _ in range(blocks)]
    for step in range(steps):
        position = step - (last - section)
        running = (position >= 0) & (position < blocks)
        flags = jnp.stack(
            [running, jnp.where(running, position, blocks), is_last, running & (section > 0)]
        ).astype(jnp.int32)
        output, kept, tok = backward_step(flags, tok, incoming, start, saved, weights, kept)
        route = [(s, s - 1) for s in range(1, sections) if 0 <= step - (last - s) < blocks]
        if route:
            incoming = lax.ppermute(output, "section", route)
        if step == 0 and relay:
            which = jnp.stack([section == 0, group // 2]).astype(jnp.int32)
            terms, tok = all_terms(which, tok, first_rows, weights, share, chunk)
        done = step - (last - 1)
        if relay and 0 <= done < blocks:
            far = shift(kept[1][done], pairs // 2, others)
            received[done][pairs // 2] = lax.ppermute(far, "section", [(s, s - 1) for s in range(1, sections)])
        done = step - last
        if relay and 0 <= done < blocks:
            mine = kept[0][done]
            received[done][0] = mine
            every = tuple(range(sections))
            for d in range(1, pairs):
                value = shift(mine, d, (last,) if d == pairs // 2 else every)
                if d == pairs // 2:
                    value = jnp.where(is_last, value, received[done][d])
                received[done][d] = value
    which = jnp.stack([(section > 0) | (not relay), group // 2]).astype(jnp.int32)
    terms, tok = all_terms(which, tok, later_rows, weights, share, chunk, terms)
    if relay:
        grad_rows = [received[b][d] for d in range(pairs) for b in range(blocks)]
    else:
        grad_rows = [kept[0][b] for b in range(blocks)]
    sums = gradients(grad_rows, terms, weights[2])
    if relay:
        core = group % 2
        results = []
        for value in sums:
            half = value.shape[0] // 2
            mine = lax.dynamic_slice_in_dim(value, core * half, half, 0)
            theirs = lax.dynamic_slice_in_dim(value, (1 - core) * half, half, 0)
            moved = lax.ppermute(theirs, "dp", [(i, i ^ 1) for i in range(groups)])
            results.append(mine.astype(F32) + moved.astype(F32))
    else:
        results = [
            lax.psum_scatter(value, "dp", scatter_dimension=0, tiled=True).astype(F32) for value in sums
        ]
    grad_gate, grad_up, grad_down = results

    embed_late = after(embed, tok)
    embed_rows = double_up(embed_late, "dp")
    sent = [lax.ppermute(embed_rows, "section", [(last, s)]) for s in range(last)]
    embed_all = jnp.where(is_last, embed_rows, functools.reduce(jnp.add, sent))
    pre_all = dot(embed_all, w_proj) + position_table(
        jnp.take(tile_pos, tile_ids), section * features, features, total
    )
    owned = slide_ids[:slides]
    member = (jnp.take(tile_slide, tile_ids)[None] == owned[:, None]).astype(F32)
    slide_embed = (
        jnp.dot(member, jax.nn.silu(pre_all), precision=lax.Precision.HIGHEST) / counts[:slides, None]
    )
    dpre_all = (back_rows(tile_ids, cot_rows) * derivative(pre_all)).astype(BF)
    own_width = width // groups
    grad_proj = dot_rows(lax.dynamic_slice_in_dim(embed_all, group * own_width, own_width, 1), dpre_all)
    return (slide_embed, grad_gate[None], grad_up[None], grad_down[None], grad_proj)


def solution(mesh):
    return jax.shard_map(
        local,
        mesh=mesh,
        in_specs=(
            P("dp", None),
            P("section", None, None),
            P("section", None, None),
            P("section", None, None),
            P(None, "section"),
            P(),
            P(),
            P("dp", "section"),
        ),
        out_specs=(
            P("dp", "section"),
            P("section", "dp", None),
            P("section", "dp", None),
            P("section", "dp", None),
            P("dp", "section"),
        ),
        check_vma=False,
    )
```
